32 devices in a mesh: dap: 32 (over z, y, x, core), ch: 1.
Axes of the slice: x: 2, y: 2, z: 4, core: 2. Of those that a mesh axis runs over, the one named last changes fastest.
Arguments:
- alignment_embedding: bfloat16 [128, 128, 256], P(None, 'dap'), may hold values from -6 to 6
- couple_embedding: bfloat16 [128, 128, 128], P('dap', 'ch'), may hold values from -6 to 6
- tensor_first_matrix: bfloat16 [256, 32], P(None, 'ch'), may hold values from -0.375 to 0.375
- tensor_second_matrix: bfloat16 [256, 32], replicated, may hold values from -0.375 to 0.375
- tensor_final_matrix: bfloat16 [1024, 128], P('ch'), may hold values from -1 to 1
- trimul_entry_matrix: bfloat16 [4, 128, 128], replicated, may hold values from -0.5 to 0.5
- trimul_sigmoid_matrix: bfloat16 [128, 128], replicated, may hold values from -0.5 to 0.5
- trimul_final_matrix: bfloat16 [128, 128], replicated, may hold values from -0.5 to 0.5
Outputs:
- pair_out: bfloat16 [128, 128, 128], P('dap', 'ch')
The draws below stay inside these ranges and needn't reach their ends.
All inputs are finite; a program needn't handle non-finite values.
Results may differ from the reference program's by a relative error of at most 0.014.
Values may be sent and summed in bfloat16 or wider, within the bound.
A program may use at most 64 MiB of HBM per device.

```python
import jax
import jax.numpy as jnp
from jax import lax

ALIGNED_SEQS = 128
ALIGNMENT_FEAT = 256
CZ = 128
PROJ_WIDTH_SIDE = 32
CT = 128
ROWS_DEV = 4
AMINO_TOTAL = 128


def block_scale(rng, extent, pieces, low, high):
    factor_of, own = 1.0, jax.random.fold_in(rng, 6)
    for position, shards_of in pieces:
        steps = jnp.exp(jax.random.uniform(jax.random.fold_in(own, position), (shards_of,), jnp.float32, low / len(pieces), high / len(pieces)))
        factor_of = factor_of * jnp.repeat(steps, extent[position] // shards_of).reshape([-1 if axis == position else 1 for axis in range(len(extent))])
    return factor_of


def scatter_about(own_key, dims, spread, bound, pieces=(), dtype=jnp.bfloat16):
    level = block_scale(own_key, dims, pieces, -0.22, 0.18) if pieces else 1.0
    values = jax.random.normal(own_key, dims, jnp.float32) * spread * level
    return jnp.minimum(jnp.maximum(values, -bound), bound).astype(dtype)


def setup_inputs(seed: int = 0) -> dict:
    splits = jax.random.split(jax.random.key(seed), 9)
    alignment_embedding = scatter_about(splits[0], (ALIGNED_SEQS, AMINO_TOTAL, ALIGNMENT_FEAT), 1.0, 6.0, ((1, 32),))
    couple_embedding = scatter_about(splits[1], (AMINO_TOTAL, AMINO_TOTAL, CZ), 1.0, 6.0, ((0, 32),))
    tensor_first_matrix = scatter_about(splits[2], (ALIGNMENT_FEAT, PROJ_WIDTH_SIDE), ALIGNMENT_FEAT ** -0.5, 0.375)
    tensor_second_matrix = scatter_about(splits[3], (ALIGNMENT_FEAT, PROJ_WIDTH_SIDE), ALIGNMENT_FEAT ** -0.5, 0.375)
    tensor_final_matrix = scatter_about(splits[4], (PROJ_WIDTH_SIDE * PROJ_WIDTH_SIDE, CZ), PROJ_WIDTH_SIDE ** -0.5, 1.0)
    trimul_entry_matrix = scatter_about(splits[5], (4, CZ, CT), CZ ** -0.5, 0.5)
    trimul_sigmoid_matrix = scatter_about(splits[6], (CZ, CZ), CZ ** -0.5, 0.5)
    trimul_final_matrix = scatter_about(splits[7], (CT, CZ), CT ** -0.5, 0.5)
    return {"alignment_embedding": alignment_embedding, "couple_embedding": couple_embedding, "tensor_first_matrix": tensor_first_matrix, "tensor_second_matrix": tensor_second_matrix, "tensor_final_matrix": tensor_final_matrix, "trimul_entry_matrix": trimul_entry_matrix, "trimul_sigmoid_matrix": trimul_sigmoid_matrix, "trimul_final_matrix": trimul_final_matrix}


def standardize_fn(value, axis):
    mean = lax.optimization_barrier(jnp.mean(value, axis=axis, keepdims=True))
    centred = value - mean
    var = lax.optimization_barrier(jnp.mean(centred * centred, axis=axis, keepdims=True))
    return centred * lax.rsqrt(var + 1e-05)

def reference(alignment_embedding, couple_embedding, tensor_first_matrix, tensor_second_matrix, tensor_final_matrix, trimul_entry_matrix, trimul_sigmoid_matrix, trimul_final_matrix):
    alignment_standardized = standardize_fn(alignment_embedding.astype(jnp.float32), -1).astype(jnp.bfloat16)
    first_operand = jnp.einsum('ziv,vl->zil', alignment_standardized.astype(jnp.float32), tensor_first_matrix.astype(jnp.float32)).astype(jnp.bfloat16)
    second_operand = jnp.einsum('ziv,vl->zil', alignment_standardized.astype(jnp.float32), tensor_second_matrix.astype(jnp.float32)).astype(jnp.bfloat16)
    blocks = AMINO_TOTAL // ROWS_DEV
    left_blocks = jnp.transpose(first_operand.reshape(ALIGNED_SEQS, blocks, ROWS_DEV, PROJ_WIDTH_SIDE), (1, 0, 2, 3))
    right32 = second_operand.astype(jnp.float32)

    def block_update(left_block):
        outer = jnp.einsum('sic,sje->ijce', left_block.astype(jnp.float32), right32) * (1.0 / ALIGNED_SEQS)
        outer = outer.astype(jnp.bfloat16).reshape(ROWS_DEV * AMINO_TOTAL, PROJ_WIDTH_SIDE * PROJ_WIDTH_SIDE)
        return jnp.dot(outer, tensor_final_matrix, preferred_element_type=jnp.float32).reshape(ROWS_DEV, AMINO_TOTAL, CZ)
    update = lax.map(block_update, left_blocks).reshape(AMINO_TOTAL, AMINO_TOTAL, CZ)
    lifted = (couple_embedding.astype(jnp.float32) + update).astype(jnp.bfloat16)
    normed = standardize_fn(lifted.astype(jnp.float32), -1).astype(jnp.bfloat16)
    flat = normed.reshape(AMINO_TOTAL * AMINO_TOTAL, CZ)
    per_channel = jnp.transpose(trimul_entry_matrix, (2, 0, 1))

    def channel_product(weights):
        proj = jnp.dot(flat, jnp.transpose(weights), preferred_element_type=jnp.float32)
        left_t = (jax.nn.sigmoid(proj[:, 0]) * proj[:, 1]).astype(jnp.bfloat16).reshape(AMINO_TOTAL, AMINO_TOTAL)
        right_t = (jax.nn.sigmoid(proj[:, 2]) * proj[:, 3]).astype(jnp.bfloat16).reshape(AMINO_TOTAL, AMINO_TOTAL)
        return jnp.dot(left_t, jnp.transpose(right_t), preferred_element_type=jnp.float32).astype(jnp.bfloat16)
    tri = lax.map(channel_product, per_channel)
    tri_n = standardize_fn(tri.astype(jnp.float32), 0).astype(jnp.bfloat16)
    out = jnp.einsum('cij,cz->ijz', tri_n.astype(jnp.float32), trimul_final_matrix.astype(jnp.float32))
    gate = jax.nn.sigmoid(jnp.dot(flat, trimul_sigmoid_matrix, preferred_element_type=jnp.float32)).reshape(AMINO_TOTAL, AMINO_TOTAL, CZ)
    return (lifted.astype(jnp.float32) + gate * out).astype(jnp.bfloat16)
```

```python
import functools

import jax
import jax.numpy as jnp
from jax import lax
from jax.experimental import pallas as pl
from jax.experimental.pallas import tpu as pltpu
from jax.sharding import PartitionSpec as P

CORES = 2
PLANE = 4


def standardize_fn(value, axis):
    mean = jnp.mean(value, axis=axis, keepdims=True)
    centred = value - mean
    var = jnp.mean(centred * centred, axis=axis, keepdims=True)
    return centred * lax.rsqrt(var + 1e-05)


def outer_update(first_operand, right_rows, w_out, alignment_height):
    rows = first_operand.shape[1]
    outer = jnp.einsum(
        "sic,sje->ijce", first_operand, right_rows, preferred_element_type=jnp.float32
    )
    outer = (outer * (1.0 / alignment_height)).astype(jnp.bfloat16)
    outer = outer.reshape(rows, right_rows.shape[1], first_operand.shape[2] * right_rows.shape[2])
    return jnp.einsum("ijf,fz->ijz", outer, w_out, preferred_element_type=jnp.float32)


def per_device(
    alignment_embedding,
    couple_embedding,
    tensor_first_matrix,
    tensor_second_matrix,
    tensor_final_matrix,
    trimul_entry_matrix,
    trimul_sigmoid_matrix,
    trimul_final_matrix,
):
    alignment_height = alignment_embedding.shape[0]
    columns = couple_embedding.shape[1]
    alignment_standardized = standardize_fn(alignment_embedding.astype(jnp.float32), -1).astype(
        jnp.bfloat16
    )
    second_operand = jnp.einsum(
        "ziv,vl->zil",
        alignment_standardized,
        tensor_second_matrix,
        preferred_element_type=jnp.float32,
    ).astype(jnp.bfloat16)
    right_all = lax.all_gather(second_operand, "dap", axis=1, tiled=True)
    first_operand = jnp.einsum(
        "ziv,vl->zil",
        alignment_standardized,
        tensor_first_matrix,
        preferred_element_type=jnp.float32,
    ).astype(jnp.bfloat16)
    terms = outer_update(first_operand, right_all, tensor_final_matrix, alignment_height)
    totals = lax.psum(terms.astype(jnp.bfloat16), "ch").astype(jnp.float32)
    update = lax.dynamic_slice_in_dim(totals, lax.axis_index("ch") * columns, columns, 1)
    lifted = (couple_embedding.astype(jnp.float32) + update).astype(jnp.bfloat16)
    normed = standardize_fn(lifted.astype(jnp.float32), -1).astype(jnp.bfloat16)
    projected = jnp.einsum(
        "rkz,qzc->qcrk", normed, trimul_entry_matrix, preferred_element_type=jnp.float32
    )
    left_t = (jax.nn.sigmoid(projected[0]) * projected[1]).astype(jnp.bfloat16)
    right_t = (jax.nn.sigmoid(projected[2]) * projected[3]).astype(jnp.bfloat16)
    left_cols, right_cols = (
        lax.all_to_all(left_t, "dap", split_axis=0, concat_axis=1, tiled=True),
        lax.all_to_all(right_t, "dap", split_axis=0, concat_axis=1, tiled=True),
    )
    product = jnp.einsum("cik,cjk->cij", left_cols, right_cols, preferred_element_type=jnp.float32)
    returned = lax.all_to_all(
        product.astype(jnp.bfloat16), "dap", split_axis=1, concat_axis=0, tiled=True
    ).astype(product.dtype)
    summed = lax.psum_scatter(returned.astype(jnp.bfloat16), "ch", scatter_dimension=2, tiled=True)
    tri_n = standardize_fn(summed.astype(jnp.float32), 0).astype(jnp.bfloat16)
    out = jnp.einsum("crj,cz->rjz", tri_n, trimul_final_matrix, preferred_element_type=jnp.float32)
    gate = jax.nn.sigmoid(
        jnp.einsum("rjz,zy->rjy", normed, trimul_sigmoid_matrix, preferred_element_type=jnp.float32)
    )
    return (lifted.astype(jnp.float32) + gate * out).astype(jnp.bfloat16)


def remote(src, dst, send_sem, recv_sem, peer):
    return pltpu.make_async_remote_copy(
        src_ref=src,
        dst_ref=dst,
        send_sem=send_sem,
        recv_sem=recv_sem,
        device_id={"dap": peer},
        device_id_type=pl.DeviceIdType.MESH,
    )


def signal(peer):
    pl.semaphore_signal(
        pltpu.get_barrier_semaphore(),
        inc=1,
        device_id={"dap": peer},
        device_id_type=pl.DeviceIdType.MESH,
    )


def gather_kernel(n, block, out, zs, zr, ps, pr, cs, cr):
    depth = n // (CORES * PLANE)
    me = lax.axis_index("dap")
    core, p, z = me % CORES, (me // CORES) % PLANE, me // (CORES * PLANE)

    def device(z_, p_, core_):
        return (z_ * PLANE + p_) * CORES + core_

    def source(zi, q):
        return device((z - zi + depth) % depth, (p - q + PLANE) % PLANE, core)

    partner = me + 1 - 2 * core
    for zi in range(1, depth):
        signal(device((z + zi) % depth, p, core))
    for q in range(1, PLANE):
        signal(device(z, (p + q) % PLANE, core))
    signal(partner)
    pl.semaphore_wait(pltpu.get_barrier_semaphore(), depth + PLANE - 1)

    copies = []

    def send(src, slot, send_sem, recv_sem, peer):
        copy = remote(src, out.at[slot], send_sem, recv_sem, peer)
        copy.start()
        copies.append(copy)
        return copy

    along = {}
    for zi in range(1, depth):
        along[zi] = send(block, me, zs.at[zi], zr.at[zi], device((z + zi) % depth, p, core))
    out[me] = block[...]
    across = {}
    for zi in range(depth):
        slot = source(zi, 0)
        if zi:
            along[zi].wait_recv()
        src = out.at[slot] if zi else block
        for q in range(1, PLANE):
            across[zi, q] = send(
                src, slot, ps.at[zi, q], pr.at[zi, q], device(z, (p + q) % PLANE, core)
            )
        across[zi, 0] = send(src, slot, cs.at[zi, 0], cr.at[zi, 0], partner)
    over = [across[zi, 0] for zi in range(depth)]
    for zi in range(depth):
        for q in range(1, PLANE):
            across[zi, q].wait_recv()
            slot = source(zi, q)
            over.append(send(out.at[slot], slot, cs.at[zi, q], cr.at[zi, q], partner))
    for copy in over:
        copy.wait_recv()
    for copy in copies:
        copy.wait_send()


def gather(block, n):
    depth = n // (CORES * PLANE)
    return pl.pallas_call(
        functools.partial(gather_kernel, n),
        out_shape=jax.ShapeDtypeStruct((n,) + block.shape, block.dtype),
        in_specs=[pl.BlockSpec(memory_space=pltpu.VMEM)],
        out_specs=pl.BlockSpec(memory_space=pltpu.VMEM),
        scratch_shapes=[
            pltpu.SemaphoreType.DMA((depth,)),
            pltpu.SemaphoreType.DMA((depth,)),
            pltpu.SemaphoreType.DMA((depth, PLANE)),
            pltpu.SemaphoreType.DMA((depth, PLANE)),
            pltpu.SemaphoreType.DMA((depth, PLANE)),
            pltpu.SemaphoreType.DMA((depth, PLANE)),
        ],
        compiler_params=pltpu.CompilerParams(collective_id=0, has_side_effects=True),
    )(block)


def triangle_kernel(n, left, right, out, lrecv, rrecv, back, ls, lr, rs, rr, bs, br):
    me = lax.axis_index("dap")
    per, rows, width = left.shape[1:]

    def greet(d, carry):
        signal((me + d) % n)
        return carry

    lax.fori_loop(1, n, greet, 0)
    pl.semaphore_wait(pltpu.get_barrier_semaphore(), n - 1)

    def there(d):
        peer = (me + d) % n
        return (
            remote(left.at[peer], lrecv.at[me], ls.at[d], lr.at[d], peer),
            remote(right.at[peer], rrecv.at[me], rs.at[d], rr.at[d], peer),
        )

    def home(d):
        peer = (me + d) % n
        return (remote(back.at[peer], out.at[me], bs.at[d], br.at[d], peer),)

    def run(make, action):
        def step(d, carry):
            for copy in make(d):
                getattr(copy, action)()
            return carry

        lax.fori_loop(1, n, step, 0)

    run(there, "start")
    lrecv[me] = left[me]
    rrecv[me] = right[me]
    run(there, "wait_recv")
    for c in range(per):
        first = lrecv[:, c].astype(jnp.float32).reshape(n * rows, width).astype(jnp.bfloat16)
        second = rrecv[:, c].astype(jnp.float32).reshape(n * rows, width).astype(jnp.bfloat16)
        product = lax.dot_general(
            first, second, (((1,), (1,)), ((), ())), preferred_element_type=jnp.float32
        )
        back[:, c] = product.reshape(n, rows, n * rows).astype(jnp.bfloat16)
    run(home, "start")
    out[me] = back[me]
    run(there, "wait_send")
    run(home, "wait_recv")
    run(home, "wait_send")


def triangle(left, right, n):
    return pl.pallas_call(
        functools.partial(triangle_kernel, n),
        out_shape=jax.ShapeDtypeStruct(left.shape, left.dtype),
        in_specs=[pl.BlockSpec(memory_space=pltpu.VMEM)] * 2,
        out_specs=pl.BlockSpec(memory_space=pltpu.VMEM),
        scratch_shapes=[pltpu.VMEM(left.shape, left.dtype)] * 3
        + [pltpu.SemaphoreType.DMA((n,))] * 6,
        compiler_params=pltpu.CompilerParams(collective_id=1, has_side_effects=True),
    )(left, right)


def per_device_direct(
    n,
    alignment_embedding,
    couple_embedding,
    tensor_first_matrix,
    tensor_second_matrix,
    tensor_final_matrix,
    trimul_entry_matrix,
    trimul_sigmoid_matrix,
    trimul_final_matrix,
):
    alignment_height, rows, _ = alignment_embedding.shape
    side = tensor_second_matrix.shape[1]
    normal = standardize_fn(alignment_embedding.astype(jnp.float32), -1).astype(jnp.bfloat16)
    block = jnp.einsum(
        "ziv,vl->ilz", normal, tensor_second_matrix, preferred_element_type=jnp.float32
    ).astype(jnp.bfloat16)
    gathered = gather(block.reshape(rows * side, alignment_height), n)
    right_rows = gathered.reshape(n * rows, side, alignment_height)
    first_operand = jnp.einsum(
        "ziv,vl->zil", normal, tensor_first_matrix, preferred_element_type=jnp.float32
    ).astype(jnp.bfloat16)
    outer = jnp.einsum(
        "sic,jes->ijce", first_operand, right_rows, preferred_element_type=jnp.float32
    )
    outer = (outer * (1.0 / alignment_height)).astype(jnp.bfloat16)
    outer = outer.reshape(rows, n * rows, -1)
    update = jnp.einsum(
        "ijf,fz->ijz", outer, tensor_final_matrix, preferred_element_type=jnp.float32
    )
    lifted = (couple_embedding.astype(jnp.float32) + update).astype(jnp.bfloat16)
    normed = standardize_fn(lifted.astype(jnp.float32), -1).astype(jnp.bfloat16)
    projected = jnp.einsum(
        "rkz,qzc->qcrk", normed, trimul_entry_matrix, preferred_element_type=jnp.float32
    )
    left_t = (jax.nn.sigmoid(projected[0]) * projected[1]).astype(jnp.bfloat16)
    right_t = (jax.nn.sigmoid(projected[2]) * projected[3]).astype(jnp.bfloat16)
    shape = (n, left_t.shape[0] // n) + left_t.shape[1:]
    returned = triangle(left_t.reshape(shape), right_t.reshape(shape), n)
    summed = returned.reshape(left_t.shape)
    tri_n = standardize_fn(summed.astype(jnp.float32), 0).astype(jnp.bfloat16)
    out = jnp.einsum("crj,cz->rjz", tri_n, trimul_final_matrix, preferred_element_type=jnp.float32)
    gate = jax.nn.sigmoid(
        jnp.einsum("rjz,zy->rjy", normed, trimul_sigmoid_matrix, preferred_element_type=jnp.float32)
    )
    return (lifted.astype(jnp.float32) + gate * out).astype(jnp.bfloat16)


def solution(mesh):
    n = mesh.shape["dap"]
    direct = mesh.shape["ch"] == 1 and n % (CORES * PLANE) == 0
    body = functools.partial(per_device_direct, n) if direct else per_device
    placed = (
        P(None, "dap", None),
        P("dap", "ch", None),
        P(None, "ch"),
        P(),
        P("ch", None),
        P(),
        P(),
        P(),
    )
    return jax.shard_map(
        body, mesh=mesh, in_specs=placed, out_specs=P("dap", "ch", None), check_vma=False
    )
```

```python
import functools

import jax
import jax.numpy as jnp
from jax import lax
from jax.experimental import pallas as pl
from jax.experimental.pallas import tpu as pltpu
from jax.sharding import PartitionSpec as P

CORES = 2
PLANE = 4


def standardize_fn(value, axis):
    mean = jnp.mean(value, axis=axis, keepdims=True)
    centred = value - mean
    var = jnp.mean(centred * centred, axis=axis, keepdims=True)
    return centred * lax.rsqrt(var + 1e-05)


def outer_update(first_operand, right_rows, w_out, alignment_height):
    rows = first_operand.shape[1]
    outer = jnp.einsum(
        "sic,sje->ijce", first_operand, right_rows, preferred_element_type=jnp.float32
    )
    outer = (outer * (1.0 / alignment_height)).astype(jnp.bfloat16)
    outer = outer.reshape(rows, right_rows.shape[1], first_operand.shape[2] * right_rows.shape[2])
    return jnp.einsum("ijf,fz->ijz", outer, w_out, preferred_element_type=jnp.float32)


def per_device(
    alignment_embedding,
    couple_embedding,
    tensor_first_matrix,
    tensor_second_matrix,
    tensor_final_matrix,
    trimul_entry_matrix,
    trimul_sigmoid_matrix,
    trimul_final_matrix,
):
    alignment_height = alignment_embedding.shape[0]
    columns = couple_embedding.shape[1]
    alignment_standardized = standardize_fn(alignment_embedding.astype(jnp.float32), -1).astype(
        jnp.bfloat16
    )
    second_operand = jnp.einsum(
        "ziv,vl->zil",
        alignment_standardized,
        tensor_second_matrix,
        preferred_element_type=jnp.float32,
    ).astype(jnp.bfloat16)
    right_all = lax.all_gather(second_operand, "dap", axis=1, tiled=True)
    first_operand = jnp.einsum(
        "ziv,vl->zil",
        alignment_standardized,
        tensor_first_matrix,
        preferred_element_type=jnp.float32,
    ).astype(jnp.bfloat16)
    terms = outer_update(first_operand, right_all, tensor_final_matrix, alignment_height)
    totals = lax.psum(terms.astype(jnp.bfloat16), "ch").astype(jnp.float32)
    update = lax.dynamic_slice_in_dim(totals, lax.axis_index("ch") * columns, columns, 1)
    lifted = (couple_embedding.astype(jnp.float32) + update).astype(jnp.bfloat16)
    normed = standardize_fn(lifted.astype(jnp.float32), -1).astype(jnp.bfloat16)
    projected = jnp.einsum(
        "rkz,qzc->qcrk", normed, trimul_entry_matrix, preferred_element_type=jnp.float32
    )
    left_t = (jax.nn.sigmoid(projected[0]) * projected[1]).astype(jnp.bfloat16)
    right_t = (jax.nn.sigmoid(projected[2]) * projected[3]).astype(jnp.bfloat16)
    left_cols, right_cols = (
        lax.all_to_all(left_t, "dap", split_axis=0, concat_axis=1, tiled=True),
        lax.all_to_all(right_t, "dap", split_axis=0, concat_axis=1, tiled=True),
    )
    product = jnp.einsum("cik,cjk->cij", left_cols, right_cols, preferred_element_type=jnp.float32)
    returned = lax.all_to_all(
        product.astype(jnp.bfloat16), "dap", split_axis=1, concat_axis=0, tiled=True
    ).astype(product.dtype)
    summed = lax.psum_scatter(returned.astype(jnp.bfloat16), "ch", scatter_dimension=2, tiled=True)
    tri_n = standardize_fn(summed.astype(jnp.float32), 0).astype(jnp.bfloat16)
    out = jnp.einsum("crj,cz->rjz", tri_n, trimul_final_matrix, preferred_element_type=jnp.float32)
    gate = jax.nn.sigmoid(
        jnp.einsum("rjz,zy->rjy", normed, trimul_sigmoid_matrix, preferred_element_type=jnp.float32)
    )
    return (lifted.astype(jnp.float32) + gate * out).astype(jnp.bfloat16)


def remote(src, dst, send_sem, recv_sem, peer):
    return pltpu.make_async_remote_copy(
        src_ref=src,
        dst_ref=dst,
        send_sem=send_sem,
        recv_sem=recv_sem,
        device_id={"dap": peer},
        device_id_type=pl.DeviceIdType.MESH,
    )


def signal(peer):
    pl.semaphore_signal(
        pltpu.get_barrier_semaphore(),
        inc=1,
        device_id={"dap": peer},
        device_id_type=pl.DeviceIdType.MESH,
    )


def normalized(value, axis):
    mean = jnp.mean(value, axis=axis, keepdims=True)
    centred = value - mean
    var = jnp.mean(centred * centred, axis=axis, keepdims=True)
    return centred * lax.rsqrt(var + 1e-05)


def fused_kernel(
    n,
    msa,
    first_t,
    second_t,
    couple_h,
    final_h,
    entry_h,
    sigmoid_h,
    output_h,
    result,
    couple,
    final,
    entry,
    sigmoid_w,
    output_w,
    rows_f32,
    final_f32,
    block,
    rall,
    rmat,
    tmat,
    lifted_s,
    gate_s,
    lsend,
    rsend,
    lrecv,
    rrecv,
    back,
    trecv,
    local,
    zs,
    zr,
    ps,
    pr,
    cs,
    cr,
    ls,
    lr,
    rs,
    rr,
    bs,
    br,
):
    f32, bf16 = jnp.float32, jnp.bfloat16
    height, rows, feat = msa.shape
    side = first_t.shape[0]
    width = couple.shape[2]
    columns = couple.shape[1]
    per = lsend.shape[1]
    depth = n // (CORES * PLANE)
    me = lax.axis_index("dap")
    core, p, z = me % CORES, (me // CORES) % PLANE, me // (CORES * PLANE)

    def greet(d, carry):
        signal((me + d) % n)
        return carry

    lax.fori_loop(1, n, greet, 0)

    loads = [
        pltpu.make_async_copy(src, dst, local.at[k])
        for k, (src, dst) in enumerate(
            (
                (final_h, final),
                (couple_h, couple),
                (entry_h, entry),
                (sigmoid_h, sigmoid_w),
                (output_h, output_w),
            )
        )
    ]
    for load in loads:
        load.start()

    x = msa[...].astype(f32).reshape(height * rows, feat)
    normal = normalized(x, -1).astype(bf16)
    weights = jnp.concatenate(
        [first_t[...], second_t[...], jnp.zeros((128 - 2 * side, feat), bf16)], axis=0
    )
    rows_f32[...] = lax.dot_general(
        normal, weights, (((1,), (1,)), ((), ())), preferred_element_type=f32
    )
    lefts = []
    rights = []
    for i in range(rows):
        both = rows_f32[pl.ds(i, height, stride=rows), :]
        lefts.append(both[:, :side].astype(bf16))
        rights.append(both.T[side : 2 * side, :])
    for i in range(rows):
        rows_f32[pl.ds(i, side, stride=rows), :] = rights[i]
    block[...] = rows_f32[pl.ds(0, side * rows), :].reshape(side, rows, height).astype(bf16)
    left_all = jnp.concatenate(lefts, axis=0)

    pl.semaphore_wait(pltpu.get_barrier_semaphore(), n - 1)

    def device(z_, p_, core_):
        return (z_ * PLANE + p_) * CORES + core_

    def source(zi, q):
        return device((z - zi + depth) % depth, (p - q + PLANE) % PLANE, core)

    partner = me + 1 - 2 * core
    copies = []

    def send(src, slot, send_sem, recv_sem, peer):
        copy = remote(src, rall.at[slot], send_sem, recv_sem, peer)
        copy.start()
        copies.append(copy)
        return copy

    along = {}
    for zi in range(1, depth):
        along[zi] = send(block, me, zs.at[zi], zr.at[zi], device((z + zi) % depth, p, core))
    across = {}

    def spread(zi, src):
        slot = source(zi, 0)
        for q in range(1, PLANE):
            across[zi, q] = send(
                src, slot, ps.at[zi, q], pr.at[zi, q], device(z, (p + q) % PLANE, core)
            )
        across[zi, 0] = send(src, slot, cs.at[zi, 0], cr.at[zi, 0], partner)

    spread(0, block)
    rall[me] = block[...]
    loads[0].wait()
    final_f32[...] = final[...].astype(f32)
    for zi in range(1, depth):
        along[zi].wait_recv()
        spread(zi, rall.at[source(zi, 0)])

    for e in range(side):
        w_e = final_f32[pl.ds(e, side, stride=side), :].astype(bf16)
        t_e = jnp.dot(left_all, w_e, preferred_element_type=f32).astype(bf16)
        for i in range(rows):
            tmat[
                i // 2, e * height : (e + 1) * height, (i % 2) * width : (i % 2 + 1) * width
            ] = t_e[i * height : (i + 1) * height]

    over = [across[zi, 0] for zi in range(depth)]
    for zi in range(depth):
        for q in range(1, PLANE):
            across[zi, q].wait_recv()
            slot = source(zi, q)
            over.append(send(rall.at[slot], slot, cs.at[zi, q], cr.at[zi, q], partner))
    for load in loads[1:]:
        load.wait()
    for copy in over:
        copy.wait_recv()

    for e in range(side):
        rmat[:, e * height : (e + 1) * height] = (
            rall[:, e].astype(f32).reshape(n * rows, height).astype(bf16)
        )
    parts = []
    for h in range(rows // 2):
        update = jnp.dot(rmat[...], tmat[h], preferred_element_type=f32) * (1.0 / height)
        for i in range(2):
            total = couple[2 * h + i].astype(f32) + update[:, i * width : (i + 1) * width]
            parts.append(total.astype(bf16))
    lifted = jnp.concatenate(parts, axis=0).astype(f32)
    lifted_s[...] = lifted
    normed = normalized(lifted, -1).astype(bf16)

    def project(q):
        return lax.dot_general(
            entry[q], normed, (((0,), (1,)), ((), ())), preferred_element_type=f32
        )

    def gated(q, dst):
        value = jax.nn.sigmoid(project(q)) * project(q + 1)
        channels = value.shape[0]
        for i in range(rows):
            rows_f32[pl.ds(i, channels, stride=rows), :] = value[
                :, i * columns : (i + 1) * columns
            ]
        dst[...] = rows_f32[...].reshape(n, per, rows, columns).astype(bf16)

    def run(make, action):
        def step(d, carry):
            getattr(make((me + d) % n, d), action)()
            return carry

        lax.fori_loop(1, n, step, 0)

    def to_left(peer, d):
        return remote(lsend.at[peer], lrecv.at[me], ls.at[d], lr.at[d], peer)

    def to_right(peer, d):
        return remote(rsend.at[peer], rrecv.at[me], rs.at[d], rr.at[d], peer)

    def home(peer, d):
        return remote(back.at[peer], trecv.at[me], bs.at[d], br.at[d], peer)

    gated(0, lsend)
    run(to_left, "start")
    gated(2, rsend)
    run(to_right, "start")
    lrecv[me] = lsend[me]
    rrecv[me] = rsend[me]
    gate_s[...] = jax.nn.sigmoid(jnp.dot(normed, sigmoid_w[...], preferred_element_type=f32))
    run(to_left, "wait_recv")
    run(to_right, "wait_recv")
    for c in range(per):
        first = lrecv[:, c].astype(f32).reshape(n * rows, columns).astype(bf16)
        second = rrecv[:, c].astype(f32).reshape(n * rows, columns).astype(bf16)
        product = lax.dot_general(
            first, second, (((1,), (1,)), ((), ())), preferred_element_type=f32
        )
        back[:, c] = product.reshape(n, rows, n * rows).astype(bf16)
    run(home, "start")
    trecv[me] = back[me]
    run(to_left, "wait_send")
    run(to_right, "wait_send")
    for copy in copies:
        copy.wait_send()
    run(home, "wait_recv")
    rows_f32[...] = trecv[...].astype(f32).reshape(n * per * rows, columns)
    for i in range(rows):
        tri = rows_f32[pl.ds(i, n * per, stride=rows), :]
        tri_n = normalized(tri, 0).astype(bf16)
        out = lax.dot_general(
            tri_n, output_w[...], (((0,), (0,)), ((), ())), preferred_element_type=f32
        )
        span = slice(i * columns, (i + 1) * columns)
        result[i] = (lifted_s[span] + gate_s[span] * out).astype(bf16)
    run(home, "wait_send")


def per_device_fused(
    n,
    alignment_embedding,
    couple_embedding,
    tensor_first_matrix,
    tensor_second_matrix,
    tensor_final_matrix,
    trimul_entry_matrix,
    trimul_sigmoid_matrix,
    trimul_final_matrix,
):
    height, rows, _ = alignment_embedding.shape
    side = tensor_second_matrix.shape[1]
    columns, width = couple_embedding.shape[1:]
    channels = trimul_entry_matrix.shape[2]
    depth = n // (CORES * PLANE)
    f32, bf16 = jnp.float32, jnp.bfloat16
    wide = (n, channels // n, rows, columns)
    late = (
        couple_embedding,
        tensor_final_matrix,
        trimul_entry_matrix,
        trimul_sigmoid_matrix,
        trimul_final_matrix,
    )
    return pl.pallas_call(
        functools.partial(fused_kernel, n),
        out_shape=jax.ShapeDtypeStruct(couple_embedding.shape, bf16),
        in_specs=[pl.BlockSpec(memory_space=pltpu.VMEM)] * 3
        + [pl.BlockSpec(memory_space=pl.ANY)] * len(late),
        out_specs=pl.BlockSpec(memory_space=pltpu.VMEM),
        scratch_shapes=[pltpu.VMEM(a.shape, a.dtype) for a in late]
        + [
            pltpu.VMEM((height * rows, 128), f32),
            pltpu.VMEM(tensor_final_matrix.shape, f32),
            pltpu.VMEM((side, rows, height), bf16),
            pltpu.VMEM((n, side, rows, height), bf16),
            pltpu.VMEM((n * rows, side * height), bf16),
            pltpu.VMEM((rows // 2, side * height, 2 * width), bf16),
            pltpu.VMEM((rows * columns, width), f32),
            pltpu.VMEM((rows * columns, width), f32),
        ]
        + [pltpu.VMEM(wide, bf16)] * 6
        + [pltpu.SemaphoreType.DMA((len(late),))]
        + [pltpu.SemaphoreType.DMA((depth,))] * 2
        + [pltpu.SemaphoreType.DMA((depth, PLANE))] * 4
        + [pltpu.SemaphoreType.DMA((n,))] * 6,
        compiler_params=pltpu.CompilerParams(collective_id=0, has_side_effects=True),
    )(
        alignment_embedding,
        tensor_first_matrix.T,
        tensor_second_matrix.T,
        *late,
    )


def solution(mesh):
    n = mesh.shape["dap"]
    direct = mesh.shape["ch"] == 1 and n % (CORES * PLANE) == 0
    body = functools.partial(per_device_fused, n) if direct else per_device
    placed = (
        P(None, "dap", None),
        P("dap", "ch", None),
        P(None, "ch"),
        P(),
        P("ch", None),
        P(),
        P(),
        P(),
    )
    return jax.shard_map(
        body, mesh=mesh, in_specs=placed, out_specs=P("dap", "ch", None), check_vma=False
    )
```

```python
import functools

import jax
import jax.numpy as jnp
from jax import lax
from jax.experimental import pallas as pl
from jax.experimental.pallas import tpu as pltpu
from jax.sharding import PartitionSpec as P

CORES = 2
PLANE = 4


def standardize_fn(value, axis):
    mean = jnp.mean(value, axis=axis, keepdims=True)
    centred = value - mean
    var = jnp.mean(centred * centred, axis=axis, keepdims=True)
    return centred * lax.rsqrt(var + 1e-05)


def outer_update(first_operand, right_rows, w_out, alignment_height):
    rows = first_operand.shape[1]
    outer = jnp.einsum(
        "sic,sje->ijce", first_operand, right_rows, preferred_element_type=jnp.float32
    )
    outer = (outer * (1.0 / alignment_height)).astype(jnp.bfloat16)
    outer = outer.reshape(rows, right_rows.shape[1], first_operand.shape[2] * right_rows.shape[2])
    return jnp.einsum("ijf,fz->ijz", outer, w_out, preferred_element_type=jnp.float32)


def per_device(
    alignment_embedding,
    couple_embedding,
    tensor_first_matrix,
    tensor_second_matrix,
    tensor_final_matrix,
    trimul_entry_matrix,
    trimul_sigmoid_matrix,
    trimul_final_matrix,
):
    alignment_height = alignment_embedding.shape[0]
    columns = couple_embedding.shape[1]
    alignment_standardized = standardize_fn(alignment_embedding.astype(jnp.float32), -1).astype(
        jnp.bfloat16
    )
    second_operand = jnp.einsum(
        "ziv,vl->zil",
        alignment_standardized,
        tensor_second_matrix,
        preferred_element_type=jnp.float32,
    ).astype(jnp.bfloat16)
    right_all = lax.all_gather(second_operand, "dap", axis=1, tiled=True)
    first_operand = jnp.einsum(
        "ziv,vl->zil",
        alignment_standardized,
        tensor_first_matrix,
        preferred_element_type=jnp.float32,
    ).astype(jnp.bfloat16)
    terms = outer_update(first_operand, right_all, tensor_final_matrix, alignment_height)
    totals = lax.psum(terms.astype(jnp.bfloat16), "ch").astype(jnp.float32)
    update = lax.dynamic_slice_in_dim(totals, lax.axis_index("ch") * columns, columns, 1)
    lifted = (couple_embedding.astype(jnp.float32) + update).astype(jnp.bfloat16)
    normed = standardize_fn(lifted.astype(jnp.float32), -1).astype(jnp.bfloat16)
    projected = jnp.einsum(
        "rkz,qzc->qcrk", normed, trimul_entry_matrix, preferred_element_type=jnp.float32
    )
    left_t = (jax.nn.sigmoid(projected[0]) * projected[1]).astype(jnp.bfloat16)
    right_t = (jax.nn.sigmoid(projected[2]) * projected[3]).astype(jnp.bfloat16)
    left_cols, right_cols = (
        lax.all_to_all(left_t, "dap", split_axis=0, concat_axis=1, tiled=True),
        lax.all_to_all(right_t, "dap", split_axis=0, concat_axis=1, tiled=True),
    )
    product = jnp.einsum("cik,cjk->cij", left_cols, right_cols, preferred_element_type=jnp.float32)
    returned = lax.all_to_all(
        product.astype(jnp.bfloat16), "dap", split_axis=1, concat_axis=0, tiled=True
    ).astype(product.dtype)
    summed = lax.psum_scatter(returned.astype(jnp.bfloat16), "ch", scatter_dimension=2, tiled=True)
    tri_n = standardize_fn(summed.astype(jnp.float32), 0).astype(jnp.bfloat16)
    out = jnp.einsum("crj,cz->rjz", tri_n, trimul_final_matrix, preferred_element_type=jnp.float32)
    gate = jax.nn.sigmoid(
        jnp.einsum("rjz,zy->rjy", normed, trimul_sigmoid_matrix, preferred_element_type=jnp.float32)
    )
    return (lifted.astype(jnp.float32) + gate * out).astype(jnp.bfloat16)


def remote(src, dst, send_sem, recv_sem, peer):
    return pltpu.make_async_remote_copy(
        src_ref=src,
        dst_ref=dst,
        send_sem=send_sem,
        recv_sem=recv_sem,
        device_id={"dap": peer},
        device_id_type=pl.DeviceIdType.MESH,
    )


def signal(peer):
    pl.semaphore_signal(
        pltpu.get_barrier_semaphore(),
        inc=1,
        device_id={"dap": peer},
        device_id_type=pl.DeviceIdType.MESH,
    )


def normalized(value, axis):
    mean = jnp.mean(value, axis=axis, keepdims=True)
    centred = value - mean
    var = jnp.mean(centred * centred, axis=axis, keepdims=True)
    return centred * lax.rsqrt(var + 1e-05)


def fused_kernel(
    n,
    msa_h,
    first_h,
    second_h,
    couple_h,
    final_h,
    entry_h,
    sigmoid_h,
    output_h,
    result,
    msa,
    first_t,
    second_t,
    couple,
    final,
    entry,
    sigmoid_w,
    output_w,
    rows_f32,
    final_f32,
    block,
    rall,
    rmat,
    tmat,
    lifted_s,
    gate_s,
    lsend,
    rsend,
    lrecv,
    rrecv,
    back,
    trecv,
    local,
    zs,
    zr,
    ps,
    pr,
    cs,
    cr,
    ls,
    lr,
    rs,
    rr,
    bs,
    br,
):
    f32, bf16 = jnp.float32, jnp.bfloat16
    height, rows, feat = msa.shape
    side = first_t.shape[0]
    width = couple.shape[2]
    columns = couple.shape[1]
    per = lsend.shape[1]
    depth = n // (CORES * PLANE)
    me = lax.axis_index("dap")
    core, p, z = me % CORES, (me // CORES) % PLANE, me // (CORES * PLANE)

    def greet(d, carry):
        signal((me + d) % n)
        return carry

    lax.fori_loop(1, n, greet, 0)

    loads = [
        pltpu.make_async_copy(src, dst, local.at[k])
        for k, (src, dst) in enumerate(
            (
                (msa_h, msa),
                (first_h, first_t),
                (second_h, second_t),
                (final_h, final),
                (couple_h, couple),
                (entry_h, entry),
                (sigmoid_h, sigmoid_w),
                (output_h, output_w),
            )
        )
    ]
    for load in loads:
        load.start()

    for load in loads[:3]:
        load.wait()
    x = msa[...].astype(f32).reshape(height * rows, feat)
    normal = normalized(x, -1).astype(bf16)
    weights = jnp.concatenate(
        [first_t[...], second_t[...], jnp.zeros((128 - 2 * side, feat), bf16)], axis=0
    )
    rows_f32[pl.ds(0, height * rows), :] = lax.dot_general(
        normal, weights, (((1,), (1,)), ((), ())), preferred_element_type=f32
    )
    lefts = []
    rights = []
    for i in range(rows):
        both = rows_f32[pl.ds(i, height, stride=rows), :]
        lefts.append(both[:, :side].astype(bf16))
        rights.append(both.T[side : 2 * side, :])
    for i in range(rows):
        rows_f32[pl.ds(i, side, stride=rows), :] = rights[i]
    block[...] = rows_f32[pl.ds(0, side * rows), :].reshape(side, rows, height).astype(bf16)
    left_all = jnp.concatenate(lefts, axis=0)

    pl.semaphore_wait(pltpu.get_barrier_semaphore(), n - 1)

    def device(z_, p_, core_):
        return (z_ * PLANE + p_) * CORES + core_

    def source(zi, q):
        return device((z - zi + depth) % depth, (p - q + PLANE) % PLANE, core)

    partner = me + 1 - 2 * core
    copies = []

    def send(src, slot, send_sem, recv_sem, peer):
        copy = remote(src, rall.at[slot], send_sem, recv_sem, peer)
        copy.start()
        copies.append(copy)
        return copy

    along = {}
    for zi in range(1, depth):
        along[zi] = send(block, me, zs.at[zi], zr.at[zi], device((z + zi) % depth, p, core))
    across = {}

    def spread(zi, src):
        slot = source(zi, 0)
        for q in range(1, PLANE):
            across[zi, q] = send(
                src, slot, ps.at[zi, q], pr.at[zi, q], device(z, (p + q) % PLANE, core)
            )
        across[zi, 0] = send(src, slot, cs.at[zi, 0], cr.at[zi, 0], partner)

    spread(0, block)
    rall[me] = block[...]
    loads[3].wait()
    final_f32[...] = final[...].astype(f32)
    for zi in range(1, depth):
        along[zi].wait_recv()
        spread(zi, rall.at[source(zi, 0)])

    for e in range(side):
        w_e = final_f32[pl.ds(e, side, stride=side), :].astype(bf16)
        t_e = jnp.dot(left_all, w_e, preferred_element_type=f32).astype(bf16)
        for i in range(rows):
            tmat[
                i // 2, e * height : (e + 1) * height, (i % 2) * width : (i % 2 + 1) * width
            ] = t_e[i * height : (i + 1) * height]

    over = [across[zi, 0] for zi in range(depth)]
    for zi in range(depth):
        for q in range(1, PLANE):
            across[zi, q].wait_recv()
            slot = source(zi, q)
            over.append(send(rall.at[slot], slot, cs.at[zi, q], cr.at[zi, q], partner))
    for load in loads[4:]:
        load.wait()
    for copy in over:
        copy.wait_recv()

    for e in range(side):
        rmat[:, e * height : (e + 1) * height] = (
            rall[:, e].astype(f32).reshape(n * rows, height).astype(bf16)
        )
    parts = []
    for h in range(rows // 2):
        update = jnp.dot(rmat[...], tmat[h], preferred_element_type=f32) * (1.0 / height)
        for i in range(2):
            total = couple[2 * h + i].astype(f32) + update[:, i * width : (i + 1) * width]
            parts.append(total.astype(bf16))
    lifted = jnp.concatenate(parts, axis=0).astype(f32)
    lifted_s[...] = lifted
    normed = normalized(lifted, -1).astype(bf16)

    def project(q):
        return lax.dot_general(
            entry[q], normed, (((0,), (1,)), ((), ())), preferred_element_type=f32
        )

    def gated(q, dst):
        value = jax.nn.sigmoid(project(q)) * project(q + 1)
        channels = value.shape[0]
        for i in range(rows):
            rows_f32[pl.ds(i, channels, stride=rows), :] = value[
                :, i * columns : (i + 1) * columns
            ]
        scattered = rows_f32[pl.ds(0, channels * rows), :]
        dst[...] = scattered.reshape(n, per, rows, columns).astype(bf16)

    def run(make, action):
        def step(d, carry):
            getattr(make((me + d) % n, d), action)()
            return carry

        lax.fori_loop(1, n, step, 0)

    def to_left(peer, d):
        return remote(lsend.at[peer], lrecv.at[me], ls.at[d], lr.at[d], peer)

    def to_right(peer, d):
        return remote(rsend.at[peer], rrecv.at[me], rs.at[d], rr.at[d], peer)

    def home(peer, d):
        return remote(back.at[peer], trecv.at[me], bs.at[d], br.at[d], peer)

    gated(0, lsend)
    run(to_left, "start")
    gated(2, rsend)
    run(to_right, "start")
    lrecv[me] = lsend[me]
    rrecv[me] = rsend[me]
    gate_s[...] = jax.nn.sigmoid(jnp.dot(normed, sigmoid_w[...], preferred_element_type=f32))
    run(to_left, "wait_recv")
    run(to_right, "wait_recv")
    for c in range(per):
        first = lrecv[:, c].astype(f32).reshape(n * rows, columns).astype(bf16)
        second = rrecv[:, c].astype(f32).reshape(n * rows, columns).astype(bf16)
        product = lax.dot_general(
            first, second, (((1,), (1,)), ((), ())), preferred_element_type=f32
        )
        back[:, c] = product.reshape(n, rows, n * rows).astype(bf16)
    run(home, "start")
    trecv[me] = back[me]
    run(to_left, "wait_send")
    run(to_right, "wait_send")
    for copy in copies:
        copy.wait_send()
    run(home, "wait_recv")
    rows_f32[pl.ds(0, n * per * rows), :] = (
        trecv[...].astype(f32).reshape(n * per * rows, columns)
    )
    for i in range(rows):
        tri = rows_f32[pl.ds(i, n * per, stride=rows), :]
        tri_n = normalized(tri, 0).astype(bf16)
        out = lax.dot_general(
            tri_n, output_w[...], (((0,), (0,)), ((), ())), preferred_element_type=f32
        )
        span = slice(i * columns, (i + 1) * columns)
        result[i] = (lifted_s[span] + gate_s[span] * out).astype(bf16)
    run(home, "wait_send")


def per_device_fused(
    n,
    alignment_embedding,
    couple_embedding,
    tensor_first_matrix,
    tensor_second_matrix,
    tensor_final_matrix,
    trimul_entry_matrix,
    trimul_sigmoid_matrix,
    trimul_final_matrix,
):
    height, rows, _ = alignment_embedding.shape
    side = tensor_second_matrix.shape[1]
    columns, width = couple_embedding.shape[1:]
    channels = trimul_entry_matrix.shape[2]
    depth = n // (CORES * PLANE)
    f32, bf16 = jnp.float32, jnp.bfloat16
    wide = (n, channels // n, rows, columns)
    operands = (
        alignment_embedding,
        tensor_first_matrix.T,
        tensor_second_matrix.T,
        couple_embedding,
        tensor_final_matrix,
        trimul_entry_matrix,
        trimul_sigmoid_matrix,
        trimul_final_matrix,
    )
    return pl.pallas_call(
        functools.partial(fused_kernel, n),
        out_shape=jax.ShapeDtypeStruct(couple_embedding.shape, bf16),
        in_specs=[pl.BlockSpec(memory_space=pl.ANY)] * len(operands),
        out_specs=pl.BlockSpec(memory_space=pltpu.VMEM),
        scratch_shapes=[pltpu.VMEM(a.shape, a.dtype) for a in operands]
        + [
            pltpu.VMEM((max(height, channels) * rows, 128), f32),
            pltpu.VMEM(tensor_final_matrix.shape, f32),
            pltpu.VMEM((side, rows, height), bf16),
            pltpu.VMEM((n, side, rows, height), bf16),
            pltpu.VMEM((n * rows, side * height), bf16),
            pltpu.VMEM((rows // 2, side * height, 2 * width), bf16),
            pltpu.VMEM((rows * columns, width), f32),
            pltpu.VMEM((rows * columns, width), f32),
        ]
        + [pltpu.VMEM(wide, bf16)] * 6
        + [pltpu.SemaphoreType.DMA((len(operands),))]
        + [pltpu.SemaphoreType.DMA((depth,))] * 2
        + [pltpu.SemaphoreType.DMA((depth, PLANE))] * 4
        + [pltpu.SemaphoreType.DMA((n,))] * 6,
        compiler_params=pltpu.CompilerParams(
            collective_id=0, has_side_effects=True
        ),
    )(*operands)


def solution(mesh):
    n = mesh.shape["dap"]
    direct = mesh.shape["ch"] == 1 and n % (CORES * PLANE) == 0
    body = functools.partial(per_device_fused, n) if direct else per_device
    placed = (
        P(None, "dap", None),
        P("dap", "ch", None),
        P(None, "ch"),
        P(),
        P("ch", None),
        P(),
        P(),
        P(),
    )
    return jax.shard_map(
        body, mesh=mesh, in_specs=placed, out_specs=P("dap", "ch", None), check_vma=False
    )
```

```python
import functools

import jax
import jax.numpy as jnp
from jax import lax
from jax.experimental import pallas as pl
from jax.experimental.pallas import tpu as pltpu
from jax.sharding import PartitionSpec as P

CORES = 2
PLANE = 4


def standardize_fn(value, axis):
    mean = jnp.mean(value, axis=axis, keepdims=True)
    centred = value - mean
    var = jnp.mean(centred * centred, axis=axis, keepdims=True)
    return centred * lax.rsqrt(var + 1e-05)


def outer_update(first_operand, right_rows, w_out, alignment_height):
    rows = first_operand.shape[1]
    outer = jnp.einsum(
        "sic,sje->ijce", first_operand, right_rows, preferred_element_type=jnp.float32
    )
    outer = (outer * (1.0 / alignment_height)).astype(jnp.bfloat16)
    outer = outer.reshape(rows, right_rows.shape[1], first_operand.shape[2] * right_rows.shape[2])
    return jnp.einsum("ijf,fz->ijz", outer, w_out, preferred_element_type=jnp.float32)


def per_device(
    alignment_embedding,
    couple_embedding,
    tensor_first_matrix,
    tensor_second_matrix,
    tensor_final_matrix,
    trimul_entry_matrix,
    trimul_sigmoid_matrix,
    trimul_final_matrix,
):
    alignment_height = alignment_embedding.shape[0]
    columns = couple_embedding.shape[1]
    alignment_standardized = standardize_fn(alignment_embedding.astype(jnp.float32), -1).astype(
        jnp.bfloat16
    )
    second_operand = jnp.einsum(
        "ziv,vl->zil",
        alignment_standardized,
        tensor_second_matrix,
        preferred_element_type=jnp.float32,
    ).astype(jnp.bfloat16)
    right_all = lax.all_gather(second_operand, "dap", axis=1, tiled=True)
    first_operand = jnp.einsum(
        "ziv,vl->zil",
        alignment_standardized,
        tensor_first_matrix,
        preferred_element_type=jnp.float32,
    ).astype(jnp.bfloat16)
    terms = outer_update(first_operand, right_all, tensor_final_matrix, alignment_height)
    totals = lax.psum(terms.astype(jnp.bfloat16), "ch").astype(jnp.float32)
    update = lax.dynamic_slice_in_dim(totals, lax.axis_index("ch") * columns, columns, 1)
    lifted = (couple_embedding.astype(jnp.float32) + update).astype(jnp.bfloat16)
    normed = standardize_fn(lifted.astype(jnp.float32), -1).astype(jnp.bfloat16)
    projected = jnp.einsum(
        "rkz,qzc->qcrk", normed, trimul_entry_matrix, preferred_element_type=jnp.float32
    )
    left_t = (jax.nn.sigmoid(projected[0]) * projected[1]).astype(jnp.bfloat16)
    right_t = (jax.nn.sigmoid(projected[2]) * projected[3]).astype(jnp.bfloat16)
    left_cols, right_cols = (
        lax.all_to_all(left_t, "dap", split_axis=0, concat_axis=1, tiled=True),
        lax.all_to_all(right_t, "dap", split_axis=0, concat_axis=1, tiled=True),
    )
    product = jnp.einsum("cik,cjk->cij", left_cols, right_cols, preferred_element_type=jnp.float32)
    returned = lax.all_to_all(
        product.astype(jnp.bfloat16), "dap", split_axis=1, concat_axis=0, tiled=True
    ).astype(product.dtype)
    summed = lax.psum_scatter(returned.astype(jnp.bfloat16), "ch", scatter_dimension=2, tiled=True)
    tri_n = standardize_fn(summed.astype(jnp.float32), 0).astype(jnp.bfloat16)
    out = jnp.einsum("crj,cz->rjz", tri_n, trimul_final_matrix, preferred_element_type=jnp.float32)
    gate = jax.nn.sigmoid(
        jnp.einsum("rjz,zy->rjy", normed, trimul_sigmoid_matrix, preferred_element_type=jnp.float32)
    )
    return (lifted.astype(jnp.float32) + gate * out).astype(jnp.bfloat16)


def remote(src, dst, send_sem, recv_sem, peer):
    return pltpu.make_async_remote_copy(
        src_ref=src,
        dst_ref=dst,
        send_sem=send_sem,
        recv_sem=recv_sem,
        device_id={"dap": peer},
        device_id_type=pl.DeviceIdType.MESH,
    )


def signal(peer):
    pl.semaphore_signal(
        pltpu.get_barrier_semaphore(),
        inc=1,
        device_id={"dap": peer},
        device_id_type=pl.DeviceIdType.MESH,
    )


def normalized(value, axis):
    mean = jnp.mean(value, axis=axis, keepdims=True)
    centred = value - mean
    var = jnp.mean(centred * centred, axis=axis, keepdims=True)
    return centred * lax.rsqrt(var + 1e-05)


def fused_kernel(
    n,
    msa_h,
    first_h,
    second_h,
    couple_h,
    final_h,
    entry_h,
    sigmoid_h,
    output_h,
    result_h,
    msa,
    first_t,
    second_t,
    couple,
    final,
    entry,
    sigmoid_w,
    output_w,
    rows_f32,
    final_f32,
    block,
    rall,
    rmat,
    tmat,
    lifted_s,
    gate_s,
    lsend,
    rsend,
    lrecv,
    rrecv,
    back,
    trecv,
    result,
    local,
    stored,
    zs,
    zr,
    ps,
    pr,
    cs,
    cr,
    ls,
    lr,
    rs,
    rr,
    bs,
    br,
):
    f32, bf16 = jnp.float32, jnp.bfloat16
    height, rows, feat = msa.shape
    side = first_t.shape[0]
    width = couple.shape[2]
    columns = couple.shape[1]
    per = lsend.shape[1]
    depth = n // (CORES * PLANE)
    me = lax.axis_index("dap")
    core, p, z = me % CORES, (me // CORES) % PLANE, me // (CORES * PLANE)

    def greet(d, carry):
        signal((me + d) % n)
        return carry

    lax.fori_loop(1, n, greet, 0)

    loads = [
        pltpu.make_async_copy(src, dst, local.at[k])
        for k, (src, dst) in enumerate(
            (
                (msa_h, msa),
                (first_h, first_t),
                (second_h, second_t),
                (final_h, final),
                (couple_h, couple),
                (entry_h, entry),
                (sigmoid_h, sigmoid_w),
                (output_h, output_w),
            )
        )
    ]
    for load in loads:
        load.start()

    for load in loads[:3]:
        load.wait()
    x = msa[...].astype(f32).reshape(height * rows, feat)
    normal = normalized(x, -1).astype(bf16)
    weights = jnp.concatenate(
        [first_t[...], second_t[...], jnp.zeros((128 - 2 * side, feat), bf16)], axis=0
    )
    rows_f32[pl.ds(0, height * rows), :] = lax.dot_general(
        normal, weights, (((1,), (1,)), ((), ())), preferred_element_type=f32
    )
    lefts = []
    rights = []
    for i in range(rows):
        both = rows_f32[pl.ds(i, height, stride=rows), :]
        lefts.append(both[:, :side].astype(bf16))
        rights.append(both.T[side : 2 * side, :])
    for i in range(rows):
        rows_f32[pl.ds(i, side, stride=rows), :] = rights[i]
    block[...] = rows_f32[pl.ds(0, side * rows), :].reshape(side, rows, height).astype(bf16)
    left_all = jnp.concatenate(lefts, axis=0)

    pl.semaphore_wait(pltpu.get_barrier_semaphore(), n - 1)

    def device(z_, p_, core_):
        return (z_ * PLANE + p_) * CORES + core_

    def source(zi, q):
        return device((z - zi + depth) % depth, (p - q + PLANE) % PLANE, core)

    partner = me + 1 - 2 * core
    copies = []

    def send(src, slot, send_sem, recv_sem, peer):
        copy = remote(src, rall.at[slot], send_sem, recv_sem, peer)
        copy.start()
        copies.append(copy)
        return copy

    along = {}
    for zi in range(1, depth):
        along[zi] = send(block, me, zs.at[zi], zr.at[zi], device((z + zi) % depth, p, core))
    across = {}

    def spread(zi, src):
        slot = source(zi, 0)
        for q in range(1, PLANE):
            across[zi, q] = send(
                src, slot, ps.at[zi, q], pr.at[zi, q], device(z, (p + q) % PLANE, core)
            )
        across[zi, 0] = send(src, slot, cs.at[zi, 0], cr.at[zi, 0], partner)

    spread(0, block)
    rall[me] = block[...]
    loads[3].wait()
    final_f32[...] = final[...].astype(f32)
    for zi in range(1, depth):
        along[zi].wait_recv()
        spread(zi, rall.at[source(zi, 0)])

    for e in range(side):
        w_e = final_f32[pl.ds(e, side, stride=side), :].astype(bf16)
        t_e = jnp.dot(left_all, w_e, preferred_element_type=f32).astype(bf16)
        for i in range(rows):
            tmat[
                i // 2, e * height : (e + 1) * height, (i % 2) * width : (i % 2 + 1) * width
            ] = t_e[i * height : (i + 1) * height]

    over = [across[zi, 0] for zi in range(depth)]
    for zi in range(depth):
        for q in range(1, PLANE):
            across[zi, q].wait_recv()
            slot = source(zi, q)
            over.append(send(rall.at[slot], slot, cs.at[zi, q], cr.at[zi, q], partner))
    for load in loads[4:]:
        load.wait()
    for copy in over:
        copy.wait_recv()

    for e in range(side):
        rmat[:, e * height : (e + 1) * height] = (
            rall[:, e].astype(f32).reshape(n * rows, height).astype(bf16)
        )
    parts = []
    for h in range(rows // 2):
        update = jnp.dot(rmat[...], tmat[h], preferred_element_type=f32) * (1.0 / height)
        for i in range(2):
            total = couple[2 * h + i].astype(f32) + update[:, i * width : (i + 1) * width]
            parts.append(total.astype(bf16))
    lifted = jnp.concatenate(parts, axis=0).astype(f32)
    lifted_s[...] = lifted
    normed = normalized(lifted, -1).astype(bf16)

    def project(q):
        return lax.dot_general(
            entry[q], normed, (((0,), (1,)), ((), ())), preferred_element_type=f32
        )

    def gated(q, dst):
        value = jax.nn.sigmoid(project(q)) * project(q + 1)
        channels = value.shape[0]
        for i in range(rows):
            rows_f32[pl.ds(i, channels, stride=rows), :] = value[
                :, i * columns : (i + 1) * columns
            ]
        scattered = rows_f32[pl.ds(0, channels * rows), :]
        dst[...] = scattered.reshape(n, per, rows, columns).astype(bf16)

    def run(make, action):
        def step(d, carry):
            getattr(make((me + d) % n, d), action)()
            return carry

        lax.fori_loop(1, n, step, 0)

    def to_left(peer, d):
        return remote(lsend.at[peer], lrecv.at[me], ls.at[d], lr.at[d], peer)

    def to_right(peer, d):
        return remote(rsend.at[peer], rrecv.at[me], rs.at[d], rr.at[d], peer)

    def home(peer, d):
        return remote(back.at[peer], trecv.at[me], bs.at[d], br.at[d], peer)

    gated(0, lsend)
    run(to_left, "start")
    gated(2, rsend)
    run(to_right, "start")
    lrecv[me] = lsend[me]
    rrecv[me] = rsend[me]
    gate_s[...] = jax.nn.sigmoid(jnp.dot(normed, sigmoid_w[...], preferred_element_type=f32))
    run(to_left, "wait_recv")
    firsts = [
        lrecv[:, c].astype(f32).reshape(n * rows, columns).astype(bf16) for c in range(per)
    ]
    run(to_right, "wait_recv")
    for c in range(per):
        first = firsts[c]
        second = rrecv[:, c].astype(f32).reshape(n * rows, columns).astype(bf16)
        product = lax.dot_general(
            first, second, (((1,), (1,)), ((), ())), preferred_element_type=f32
        )
        back[:, c] = product.reshape(n, rows, n * rows).astype(bf16)
    run(home, "start")
    trecv[me] = back[me]
    run(to_left, "wait_send")
    run(to_right, "wait_send")
    for copy in copies:
        copy.wait_send()
    run(home, "wait_recv")
    rows_f32[pl.ds(0, n * per * rows), :] = (
        trecv[...].astype(f32).reshape(n * per * rows, columns)
    )
    stores = []
    for i in range(rows):
        tri = rows_f32[pl.ds(i, n * per, stride=rows), :]
        tri_n = normalized(tri, 0).astype(bf16)
        out = lax.dot_general(
            tri_n, output_w[...], (((0,), (0,)), ((), ())), preferred_element_type=f32
        )
        span = slice(i * columns, (i + 1) * columns)
        result[i] = (lifted_s[span] + gate_s[span] * out).astype(bf16)
        stores.append(pltpu.make_async_copy(result.at[i], result_h.at[i], stored.at[i]))
        stores[-1].start()
    run(home, "wait_send")
    for store in stores:
        store.wait()


def per_device_fused(
    n,
    alignment_embedding,
    couple_embedding,
    tensor_first_matrix,
    tensor_second_matrix,
    tensor_final_matrix,
    trimul_entry_matrix,
    trimul_sigmoid_matrix,
    trimul_final_matrix,
):
    height, rows, _ = alignment_embedding.shape
    side = tensor_second_matrix.shape[1]
    columns, width = couple_embedding.shape[1:]
    channels = trimul_entry_matrix.shape[2]
    depth = n // (CORES * PLANE)
    f32, bf16 = jnp.float32, jnp.bfloat16
    wide = (n, channels // n, rows, columns)
    operands = (
        alignment_embedding,
        tensor_first_matrix.T,
        tensor_second_matrix.T,
        couple_embedding,
        tensor_final_matrix,
        trimul_entry_matrix,
        trimul_sigmoid_matrix,
        trimul_final_matrix,
    )
    return pl.pallas_call(
        functools.partial(fused_kernel, n),
        out_shape=jax.ShapeDtypeStruct(couple_embedding.shape, bf16),
        in_specs=[pl.BlockSpec(memory_space=pl.ANY)] * len(operands),
        out_specs=pl.BlockSpec(memory_space=pl.ANY),
        scratch_shapes=[pltpu.VMEM(a.shape, a.dtype) for a in operands]
        + [
            pltpu.VMEM((max(height, channels) * rows, 128), f32),
            pltpu.VMEM(tensor_final_matrix.shape, f32),
            pltpu.VMEM((side, rows, height), bf16),
            pltpu.VMEM((n, side, rows, height), bf16),
            pltpu.VMEM((n * rows, side * height), bf16),
            pltpu.VMEM((rows // 2, side * height, 2 * width), bf16),
            pltpu.VMEM((rows * columns, width), f32),
            pltpu.VMEM((rows * columns, width), f32),
        ]
        + [pltpu.VMEM(wide, bf16)] * 6
        + [pltpu.VMEM(couple_embedding.shape, bf16)]
        + [pltpu.SemaphoreType.DMA((len(operands),))]
        + [pltpu.SemaphoreType.DMA((rows,))]
        + [pltpu.SemaphoreType.DMA((depth,))] * 2
        + [pltpu.SemaphoreType.DMA((depth, PLANE))] * 4
        + [pltpu.SemaphoreType.DMA((n,))] * 6,
        compiler_params=pltpu.CompilerParams(
            collective_id=0, has_side_effects=True
        ),
    )(*operands)


def solution(mesh):
    n = mesh.shape["dap"]
    direct = mesh.shape["ch"] == 1 and n % (CORES * PLANE) == 0
    body = functools.partial(per_device_fused, n) if direct else per_device
    placed = (
        P(None, "dap", None),
        P("dap", "ch", None),
        P(None, "ch"),
        P(),
        P("ch", None),
        P(),
        P(),
        P(),
    )
    return jax.shard_map(
        body, mesh=mesh, in_specs=placed, out_specs=P("dap", "ch", None), check_vma=False
    )
```
